32 devices in a mesh: row: 8 (over z, x), col: 4 (over y, core).
Axes of the slice: x: 2, y: 2, z: 4, core: 2. Of those that a mesh axis runs over, the one named last changes fastest.
Arguments:
- ztrail: float32 [4096, 4096], P('row', 'col'), may hold values from -32 to 32
- panels: float32 [4096, 1024], P('row', 'col'), may hold values from -0.1875 to 0.1875
- window_tiles: float32 [3, 512, 512], P(None, 'row'), may hold values from -3 to 3, as said below
Outputs:
- first_column: float32 [4096, 512], P(('row', 'col'))
- second_column: float32 [4096, 512], P(('row', 'col'))
- corner: float32 [3, 512, 512], P(None, 'row', 'col')
The draws below stay inside these ranges and needn't reach their ends.
Inputs may be any that keep to these rules, and one draw needn't show every extreme that they name: window_tiles[0] and window_tiles[1] are lower triangular with diagonal entries between 1 and 3.
All inputs are finite; a program needn't handle non-finite values.
Results may differ from the reference program's by a relative error of at most 0.00026.
Values sent between devices are 32-bit elements; how exact they have to be, the bound alone decides.
A program may use at most 64 MiB of HBM per device.

```python
import math
import jax
import jax.numpy as jnp
from jax import lax

TILE = 512
TRAIL = 4096


def draw_ztrail(key, part):
    key_normal, key_diag = jax.random.split(jax.random.fold_in(key, 17), 2)
    gaussian = jnp.clip(jax.random.normal(key_normal, (TRAIL, TRAIL), jnp.float32), -6.0, 6.0)
    coupled = (gaussian + gaussian.T) * (math.sqrt(0.5) / math.sqrt(TRAIL))
    diagonal = jax.random.uniform(key_diag, (TRAIL,), jnp.float32, 0.5, 2.0)
    matrix = coupled + jnp.diag(diagonal)
    return matrix


def draw_window_tiles(key, part):
    key_diag, key_lower, key_couple = jax.random.split(jax.random.fold_in(key, 23), 3)
    width = TILE
    diagonal = jax.random.uniform(key_diag, (2, width), jnp.float32, 1.0, 2.0)
    lower = jnp.clip(jax.random.normal(key_lower, (2, width, width), jnp.float32), -4.0, 4.0) * (0.5 / math.sqrt(width))
    lower = jnp.tril(lower, -1) + diagonal[:, :, None] * jnp.eye(width, dtype=jnp.float32)[None, :, :]
    coupling = jnp.clip(jax.random.normal(key_couple, (1, width, width), jnp.float32), -4.0, 4.0) / math.sqrt(width)
    return jnp.concatenate([lower, coupling], axis=0)


def block_scale(own_key, dims, cuts, least, largest):
    loudness = 1.0
    for position, shards_of in cuts:
        steps = jax.random.uniform(jax.random.fold_in(jax.random.fold_in(own_key, 6), position), (shards_of,), jnp.float32, least / len(cuts), largest / len(cuts))
        loudness = loudness * jnp.repeat(jnp.exp(steps), dims[position] // shards_of).reshape((-1,) + (1,) * (len(dims) - 1 - position))
    return loudness


def scatter_about(rng, dims, scale, most, shards=(), held_as=jnp.bfloat16):
    loudness = block_scale(rng, dims, shards, -0.22, 0.18) if shards else 1.0
    array = jax.random.normal(rng, dims, jnp.float32) * scale * loudness
    return jnp.minimum(jnp.maximum(array, -most), most).astype(held_as)


def setup_inputs(seed: int = 0) -> dict:
    key_of = jax.random.split(jax.random.key(seed), 4)
    ztrail = draw_ztrail(jax.random.fold_in(key_of[3], 71), 0)
    panels = scatter_about(key_of[1], (TRAIL, 2 * TILE), (TRAIL // 4) ** -0.5, 0.1875, ((0, 8), (1, 4)), jnp.float32)
    window_tiles = draw_window_tiles(jax.random.fold_in(key_of[3], 71), 0)
    return {"ztrail": ztrail, "panels": panels, "window_tiles": window_tiles}


def matmul(left_side, right_side):
    return jnp.dot(left_side.astype(jnp.float32), right_side.astype(jnp.float32), precision=lax.Precision.HIGHEST, preferred_element_type=jnp.float32)

def inner_rows(left_rows, right_rows):
    return lax.dot_general(left_rows.astype(jnp.float32), right_rows.astype(jnp.float32), (((0,), (0,)), ((), ())), precision=lax.Precision.HIGHEST, preferred_element_type=jnp.float32)

def right_solve(right_side, lower_tile):
    return lax.linalg.triangular_solve(lower_tile, right_side, left_side=False, lower=True)

def left_solve_t(right_side, lower_tile):
    return lax.linalg.triangular_solve(lower_tile, right_side, left_side=True, lower=True, transpose_a=True)

def corner_tiles(pivot_first, pivot_second, coupling, gram_aa, gram_ab, gram_bb):
    identity = jnp.eye(pivot_first.shape[0], dtype=jnp.float32)
    tile_aa = left_solve_t(right_solve(identity + gram_aa, pivot_first), pivot_first)
    weighed = left_solve_t(gram_ab, pivot_first)
    tile_ab = -right_solve(matmul(tile_aa, coupling) - weighed, pivot_second)
    inner = left_solve_t(identity + gram_bb - inner_rows(coupling, weighed), pivot_second)
    tile_bb = right_solve(inner - inner_rows(tile_ab, coupling), pivot_second)
    return jnp.stack([tile_aa, tile_ab, tile_bb], axis=0)

def reference(ztrail, panels, window_tiles):
    pivot_first = window_tiles[0]
    pivot_second = window_tiles[1]
    coupling = window_tiles[2]
    images = matmul(ztrail, panels)
    first_column = -right_solve(images[:, :TILE], pivot_first)
    second_column = -right_solve(images[:, TILE:] + matmul(first_column, coupling), pivot_second)
    gram_aa = inner_rows(panels[:, :TILE], images[:, :TILE])
    gram_ab = inner_rows(panels[:, :TILE], images[:, TILE:])
    gram_bb = inner_rows(panels[:, TILE:], images[:, TILE:])
    corner = corner_tiles(pivot_first, pivot_second, coupling, gram_aa, gram_ab, gram_bb)
    return (first_column, second_column, corner)
```

```python
import functools

import jax
import jax.numpy as jnp
from jax import lax
from jax.experimental import pallas as pl
from jax.experimental.pallas import tpu as pltpu
from jax.sharding import PartitionSpec as P

HIGHEST = lax.Precision.HIGHEST
HIGH = lax.Precision.HIGH
MESH = pl.DeviceIdType.MESH
VMEM_SPEC = pl.BlockSpec(memory_space=pltpu.VMEM)
VMEM_BYTES = 48 * 1024 * 1024


def dot(left, right, dims=((1,), (0,)), precision=HIGH):
    return lax.dot_general(
        left, right, (dims, ((), ())), precision=precision, preferred_element_type=jnp.float32
    )


def gather_kernel(
    cols, group, halves, p_ref, far_ref, own_ref, zbuf,
    zsend, zrecv, ysend, yrecv, xsend, xrecv, osend, orecv,
):
    rows, width = p_ref.shape
    part = rows // halves
    r = lax.axis_index("row")
    c = lax.axis_index("col")
    g = r // group
    j = r % group
    flat = width % 128 == 0

    def slot(ref, column):
        if flat:
            return ref.at[:, pl.ds(pl.multiple_of(column * width, width), width)]
        return ref.at[column]

    def far_at(jj, column, h):
        return slot(far_ref.at[jj], column).at[pl.ds(h * part, part)]

    barrier = pltpu.get_barrier_semaphore()

    def greet(row, col):
        pl.semaphore_signal(barrier, inc=1, device_id=(row, col), device_id_type=MESH)

    for k in range(1, cols):
        greet(r, (c + k) % cols)
    for k in range(1, group):
        greet(g * group + (j + k) % group, c)
    has_left = g > 0
    has_right = g < cols - 1
    pl.when(has_left)(lambda: greet(r - group, c))
    pl.when(has_right)(lambda: greet(r + group, c))
    edges = has_left.astype(jnp.int32) + has_right.astype(jnp.int32)
    pl.semaphore_wait(barrier, cols - 1 + group - 1 + edges)

    pending = []

    def send(cond, src, dst, ssem, rsem, row, col):
        copy = pltpu.make_async_remote_copy(
            src_ref=src, dst_ref=dst, send_sem=ssem, recv_sem=rsem,
            device_id=(row, col), device_id_type=MESH,
        )
        if cond is None:
            copy.start()
        else:
            pl.when(cond)(copy.start)
        pending.append((cond, copy))

    def await_recv(dst, rsem):
        pltpu.make_async_copy(dst, dst, rsem).wait()

    def spread_x(cond, src, column, h):
        for k in range(1, group):
            jj = (j + k) % group
            send(cond, src, far_at(j, column, h), xsend.at[k, column, h],
                 xrecv.at[j, column, h], g * group + jj, c)

    def deliver(cond, src, gs, h):
        remote = gs != c
        local = gs == c
        if cond is not None:
            remote = jnp.logical_and(cond, remote)
            local = jnp.logical_and(cond, local)
        send(remote, src, far_at(j, c, h), ysend.at[gs, h], yrecv.at[c, h], r, gs)
        spread_x(local, src, c, h)

        def keep():
            far_at(j, c, h)[...] = src[...]

        pl.when(local)(keep)

    def relay_x(step):
        mine = jnp.logical_or(g - step == c, g + step == c)
        for h in range(halves):
            for k in range(1, cols):
                column = (c + k) % cols
                block = far_at(j, column, h)
                pl.when(mine)(functools.partial(await_recv, block, yrecv.at[column, h]))
                spread_x(mine, block, column, h)

    for h in range(halves):
        block = p_ref.at[pl.ds(h * part, part)]
        send(has_right, block, zbuf.at[g, pl.ds(h * part, part)], zsend.at[0, g, h],
             zrecv.at[g, h], r + group, c)
        send(has_left, block, zbuf.at[g, pl.ds(h * part, part)], zsend.at[1, g, h],
             zrecv.at[g, h], r - group, c)
    for h in range(halves):
        deliver(None, p_ref.at[pl.ds(h * part, part)], g, h)
    for step in range(1, cols):
        for h in range(halves):
            for side in range(2):
                gs = g - step if side == 0 else g + step
                there = gs >= 0 if side == 0 else gs < cols
                onward = jnp.logical_and(there, has_right if side == 0 else has_left)
                gs = jnp.clip(gs, 0, cols - 1)
                block = zbuf.at[gs, pl.ds(h * part, part)]
                pl.when(there)(functools.partial(await_recv, block, zrecv.at[gs, h]))
                send(onward, block, block, zsend.at[side, gs, h], zrecv.at[gs, h],
                     r + group if side == 0 else r - group, c)
                deliver(there, block, gs, h)
        if step == 1:
            for k in range(1, cols):
                send(None, p_ref, slot(own_ref, c), osend.at[k], orecv.at[c], r, (c + k) % cols)
            slot(own_ref, c)[...] = p_ref[...]
        relay_x(step - 1)
    relay_x(cols - 1)
    for k in range(1, cols):
        column = (c + k) % cols
        await_recv(slot(own_ref, column), orecv.at[column])
    for k in range(1, group):
        jj = (j + k) % group
        for column in range(cols):
            for h in range(halves):
                await_recv(far_at(jj, column, h), xrecv.at[jj, column, h])
    for cond, copy in pending:
        if cond is None:
            copy.wait_send()
        else:
            pl.when(cond)(copy.wait_send)


def gather_panels(panels, row_total, cols):
    rows, width = panels.shape
    group = row_total // cols
    halves = 2
    flat = width % 128 == 0
    shape = (rows, cols * width) if flat else (cols, rows, width)
    dma = pltpu.SemaphoreType.DMA
    far, own = pl.pallas_call(
        functools.partial(gather_kernel, cols, group, halves),
        out_shape=(
            jax.ShapeDtypeStruct((group,) + shape, jnp.float32),
            jax.ShapeDtypeStruct(shape, jnp.float32),
        ),
        in_specs=[VMEM_SPEC],
        out_specs=(VMEM_SPEC, VMEM_SPEC),
        scratch_shapes=[
            pltpu.VMEM((cols, rows, width), jnp.float32),
            dma((2, cols, halves)),
            dma((cols, halves)),
            dma((cols, halves)),
            dma((cols, halves)),
            dma((group, cols, halves)),
            dma((group, cols, halves)),
            dma((cols,)),
            dma((cols,)),
        ],
        compiler_params=pltpu.CompilerParams(
            collective_id=0, has_side_effects=True, vmem_limit_bytes=VMEM_BYTES
        ),
    )(panels)
    if not flat:
        far = jnp.swapaxes(far, 1, 2)
        own = jnp.swapaxes(own, 0, 1)
    return far.reshape(group * rows, cols * width), own.reshape(rows, cols * width)


def exchange_kernel(axis, total, add, x_ref, out_ref, held, send_sem, recv_sem):
    me = lax.axis_index(axis)
    barrier = pltpu.get_barrier_semaphore()
    for k in range(1, total):
        pl.semaphore_signal(
            barrier, inc=1, device_id={axis: (me + k) % total}, device_id_type=MESH
        )
    pl.semaphore_wait(barrier, total - 1)
    copies = []
    for k in range(1, total):
        to = (me + k) % total
        copy = pltpu.make_async_remote_copy(
            src_ref=x_ref.at[to], dst_ref=held.at[k - 1], send_sem=send_sem.at[k - 1],
            recv_sem=recv_sem.at[k - 1], device_id={axis: to}, device_id_type=MESH,
        )
        copy.start()
        copies.append(copy)
    if add:
        out_ref[...] = x_ref[me]
    else:
        out_ref[me] = x_ref[me]
    for k in range(1, total):
        copies[k - 1].wait_recv()
        if add:
            out_ref[...] += held[k - 1]
        else:
            out_ref[(me + total - k) % total] = held[k - 1]
    for copy in copies:
        copy.wait_send()


def exchange(x, axis, add, collective_id):
    total = x.shape[0]
    out = x.shape[1:] if add else x.shape
    return pl.pallas_call(
        functools.partial(exchange_kernel, axis, total, add),
        out_shape=jax.ShapeDtypeStruct(out, jnp.float32),
        in_specs=[VMEM_SPEC],
        out_specs=VMEM_SPEC,
        scratch_shapes=[
            pltpu.VMEM((total - 1,) + x.shape[1:], jnp.float32),
            pltpu.SemaphoreType.DMA((total - 1,)),
            pltpu.SemaphoreType.DMA((total - 1,)),
        ],
        compiler_params=pltpu.CompilerParams(
            collective_id=collective_id, has_side_effects=True, vmem_limit_bytes=VMEM_BYTES
        ),
    )(x)


def batched(left, right):
    return lax.dot_general(
        left, right, (((2,), (1,)), ((0,), (0,))), precision=HIGHEST,
        preferred_element_type=jnp.float32,
    )


def lower_inverses(tiles):
    count, width, _ = tiles.shape
    base = min(128, width)
    blocks = width // base
    diag = jnp.concatenate(
        [tiles[:, i * base : (i + 1) * base, i * base : (i + 1) * base] for i in range(blocks)], 0
    )
    at_row = lax.broadcasted_iota(jnp.int32, (base, base), 0)
    at_col = lax.broadcasted_iota(jnp.int32, (base, base), 1)
    eye = (at_row == at_col).astype(jnp.float32)
    recip = 1.0 / jnp.sum(diag * eye, axis=2)

    def below(size):
        return jnp.logical_and(at_row // (2 * size) == at_col // (2 * size),
                               jnp.logical_and((at_row // size) % 2 == 1, (at_col // size) % 2 == 0))

    inverse = eye * recip[:, None, :] - jnp.where(below(1), diag, 0.0) * (
        recip[:, :, None] * recip[:, None, :]
    )
    size = 2
    while size < base:
        inverse = inverse - batched(batched(inverse, jnp.where(below(size), diag, 0.0)), inverse)
        size *= 2
    parts = [inverse[i * count : (i + 1) * count] for i in range(blocks)]
    while len(parts) > 1:
        wide = parts[0].shape[1]
        merged = []
        for i in range(0, len(parts), 2):
            low = tiles[:, (i + 1) * wide : (i + 2) * wide, i * wide : (i + 1) * wide]
            corner = -batched(batched(parts[i + 1], low), parts[i])
            top = jnp.concatenate([parts[i], jnp.zeros_like(corner)], 2)
            merged.append(jnp.concatenate([top, jnp.concatenate([corner, parts[i + 1]], 2)], 1))
        parts = merged
    return parts[0]


def local(ztrail, panels, window_tiles):
    window = lax.all_gather(window_tiles, "row", axis=1, tiled=True)
    tile = window.shape[1]
    row_total = lax.axis_size("row")
    cols = lax.axis_size("col")
    col_index = lax.axis_index("col")
    far_rows, own_rows = gather_panels(panels, row_total, cols)

    inverses = lower_inverses(window[:2])
    inv_a = inverses[0]
    inv_b = inverses[1]
    inv_ab = -dot(dot(inv_a, window[2], precision=HIGHEST), inv_b, precision=HIGHEST)
    second = jnp.concatenate([inv_ab, inv_b], axis=0)

    partial = dot(ztrail, far_rows)
    share = partial.shape[0] // cols
    images = exchange(partial.reshape(cols, share, 2 * tile), "col", True, 1)
    solved_a = dot(images[:, :tile], inv_a)
    solved_b = dot(images, second)

    block = tile // cols
    solved = jnp.stack([solved_a.reshape(share, cols, block), solved_b.reshape(share, cols, block)], 2)
    solved = jnp.swapaxes(solved.reshape(share, cols, 2 * block), 0, 1)
    row_solved = exchange(solved, "col", False, 2).reshape(cols * share, 2 * block)

    def cut(array):
        return lax.dynamic_slice_in_dim(array, col_index * block, block, 1)

    part = 1.0 / row_total
    cut_ab = cut(inv_ab) * part
    inner_a = dot(own_rows[:, :tile], row_solved, ((0,), (0,)))
    inner_a = inner_a + jnp.concatenate([cut(inv_a) * part, cut_ab], 1)
    inner_b = dot(own_rows[:, tile:], row_solved[:, block:], ((0,), (0,))) + cut(inv_b) * part
    tiles_a = dot(inv_a, inner_a, ((0,), (0,)))
    tile_bb = dot(second, jnp.concatenate([inner_a[:, block:], inner_b], 0), ((0,), (0,)))
    corner = jnp.stack([tiles_a[:, :block], tiles_a[:, block:], tile_bb], 0)
    corner = corner.reshape(3, row_total, tile // row_total, block)
    corner_block = exchange(jnp.swapaxes(corner, 0, 1), "row", True, 3)
    return (-solved_a, -solved_b, corner_block)


def solution(mesh):
    placed = (P("row", "col"), P("row", "col"), P(None, "row", None))
    return jax.shard_map(
        local,
        mesh=mesh,
        in_specs=placed,
        out_specs=(P(("row", "col"), None), P(("row", "col"), None), P(None, "row", "col")),
        check_vma=False,
    )
```

```python
import functools

import jax
import jax.numpy as jnp
from jax import lax
from jax.experimental import pallas as pl
from jax.experimental.pallas import tpu as pltpu
from jax.sharding import PartitionSpec as P

HIGHEST = lax.Precision.HIGHEST
HIGH = lax.Precision.HIGH
MESH = pl.DeviceIdType.MESH
VMEM_SPEC = pl.BlockSpec(memory_space=pltpu.VMEM)
VMEM_BYTES = 48 * 1024 * 1024


def dot(left, right, dims=((1,), (0,)), precision=HIGH):
    return lax.dot_general(
        left, right, (dims, ((), ())), precision=precision, preferred_element_type=jnp.float32
    )


def gather_kernel(
    cols, group, halves, p_ref, w_ref, far_ref, own_ref, win_ref, zbuf,
    zsend, zrecv, ysend, yrecv, xsend, xrecv, osend, orecv, ofwd,
    wzsend, wzrecv, wxsend, wxrecv, wdsend, wdrecv,
):
    rows, width = p_ref.shape
    part = rows // halves
    r = lax.axis_index("row")
    c = lax.axis_index("col")
    g = r // group
    j = r % group
    flat = width % 128 == 0

    def slot(ref, column):
        if flat:
            return ref.at[:, pl.ds(pl.multiple_of(column * width, width), width)]
        return ref.at[column]

    def far_at(jj, column, h):
        return slot(far_ref.at[jj], column).at[pl.ds(h * part, part)]

    barrier = pltpu.get_barrier_semaphore()

    def greet(row, col):
        pl.semaphore_signal(barrier, inc=1, device_id=(row, col), device_id_type=MESH)

    for k in range(1, cols):
        greet(r, (c + k) % cols)
    for k in range(1, group):
        greet(g * group + (j + k) % group, c)
    has_left = g > 0
    has_right = g < cols - 1
    pl.when(has_left)(lambda: greet(r - group, c))
    pl.when(has_right)(lambda: greet(r + group, c))
    edges = has_left.astype(jnp.int32) + has_right.astype(jnp.int32)
    pl.semaphore_wait(barrier, cols - 1 + group - 1 + edges)

    pending = []

    def send(cond, src, dst, ssem, rsem, row, col):
        copy = pltpu.make_async_remote_copy(
            src_ref=src, dst_ref=dst, send_sem=ssem, recv_sem=rsem,
            device_id=(row, col), device_id_type=MESH,
        )
        if cond is None:
            copy.start()
        else:
            pl.when(cond)(copy.start)
        pending.append((cond, copy))

    def await_recv(dst, rsem):
        pltpu.make_async_copy(dst, dst, rsem).wait()

    def spread_x(cond, src, column, h):
        for k in range(1, group):
            jj = (j + k) % group
            send(cond, src, far_at(j, column, h), xsend.at[k, column, h],
                 xrecv.at[j, column, h], g * group + jj, c)

    def deliver(cond, src, gs, h):
        remote = gs != c
        local = gs == c
        if cond is not None:
            remote = jnp.logical_and(cond, remote)
            local = jnp.logical_and(cond, local)
        send(remote, src, far_at(j, c, h), ysend.at[gs, h], yrecv.at[c, h], r, gs)
        spread_x(local, src, c, h)

        def keep():
            far_at(j, c, h)[...] = src[...]

        pl.when(local)(keep)

    def relay_x(step):
        mine = jnp.logical_or(g - step == c, g + step == c)
        for h in range(halves):
            for k in range(1, cols):
                column = (c + k) % cols
                block = far_at(j, column, h)
                pl.when(mine)(functools.partial(await_recv, block, yrecv.at[column, h]))
                spread_x(mine, block, column, h)

    for h in range(halves):
        block = p_ref.at[pl.ds(h * part, part)]
        send(has_right, block, zbuf.at[g, pl.ds(h * part, part)], zsend.at[0, g, h],
             zrecv.at[g, h], r + group, c)
        send(has_left, block, zbuf.at[g, pl.ds(h * part, part)], zsend.at[1, g, h],
             zrecv.at[g, h], r - group, c)
    for h in range(halves):
        deliver(None, p_ref.at[pl.ds(h * part, part)], g, h)

    parity = c % 2
    mate = c + 1 - 2 * parity
    tall = w_ref.shape[1]
    half_lanes = w_ref.shape[2] // 2

    def lanes(side):
        return pl.ds(pl.multiple_of(side * half_lanes, half_lanes), half_lanes)

    def win_at(gg, jj, side):
        start = pl.multiple_of((gg * group + jj) * tall, tall)
        return win_ref.at[:, pl.ds(start, tall), lanes(side)]

    def spread_win(cond, src, gg):
        for k in range(1, group):
            send(cond, src, win_at(gg, j, parity), wxsend.at[k, gg], wxrecv.at[j, gg],
                 g * group + (j + k) % group, c)

    own_win = w_ref.at[:, :, lanes(parity)]
    send(has_right, own_win, win_at(g, j, parity), wzsend.at[0, g], wzrecv.at[g], r + group, c)
    send(has_left, own_win, win_at(g, j, parity), wzsend.at[1, g], wzrecv.at[g], r - group, c)
    spread_win(None, own_win, g)
    win_ref[:, pl.ds(pl.multiple_of(r * tall, tall), tall), :] = w_ref[...]
    for step in range(1, cols):
        for h in range(halves):
            for side in range(2):
                gs = g - step if side == 0 else g + step
                there = gs >= 0 if side == 0 else gs < cols
                onward = jnp.logical_and(there, has_right if side == 0 else has_left)
                gs = jnp.clip(gs, 0, cols - 1)
                block = zbuf.at[gs, pl.ds(h * part, part)]
                pl.when(there)(functools.partial(await_recv, block, zrecv.at[gs, h]))
                send(onward, block, block, zsend.at[side, gs, h], zrecv.at[gs, h],
                     r + group if side == 0 else r - group, c)
                deliver(there, block, gs, h)
        if step == 1:
            for k in range(0, cols, 2):
                to = (c + k) % cols if k else mate
                send(None, p_ref, slot(own_ref, c), osend.at[k], orecv.at[c], r, to)
            slot(own_ref, c)[...] = p_ref[...]
        for side in range(2):
            gs = g - step if side == 0 else g + step
            there = gs >= 0 if side == 0 else gs < cols
            onward = jnp.logical_and(there, has_right if side == 0 else has_left)
            gs = jnp.clip(gs, 0, cols - 1)
            block = win_at(gs, j, parity)
            pl.when(there)(functools.partial(await_recv, block, wzrecv.at[gs]))
            send(onward, block, block, wzsend.at[side, gs], wzrecv.at[gs],
                 r + group if side == 0 else r - group, c)
            spread_win(there, block, gs)
            send(there, block, block, wdsend.at[j, gs], wdrecv.at[j, gs], r, mate)
        relay_x(step - 1)
    relay_x(cols - 1)
    for k in range(2, cols, 2):
        column = (c + k) % cols
        block = slot(own_ref, column)
        await_recv(block, orecv.at[column])
        send(None, block, block, ofwd.at[column], orecv.at[column], r, mate)
    for k in range(1, group):
        jj = (j + k) % group
        for gg in range(cols):
            block = win_at(gg, jj, parity)
            await_recv(block, wxrecv.at[jj, gg])
            send(None, block, block, wdsend.at[jj, gg], wdrecv.at[jj, gg], r, mate)
    for k in range(0, cols, 2):
        column = (mate + k) % cols
        await_recv(slot(own_ref, column), orecv.at[column])
    for k in range(1, cols):
        gg = (g + k) % cols
        await_recv(win_at(gg, j, 1 - parity), wdrecv.at[j, gg])
    for k in range(1, group):
        jj = (j + k) % group
        for gg in range(cols):
            await_recv(win_at(gg, jj, 1 - parity), wdrecv.at[jj, gg])
    for k in range(1, group):
        jj = (j + k) % group
        for column in range(cols):
            for h in range(halves):
                await_recv(far_at(jj, column, h), xrecv.at[jj, column, h])
    for cond, copy in pending:
        if cond is None:
            copy.wait_send()
        else:
            pl.when(cond)(copy.wait_send)


def gather_all(panels, window, row_total, cols):
    rows, width = panels.shape
    deep, tall, tile = window.shape
    group = row_total // cols
    halves = 2
    flat = width % 128 == 0
    shape = (rows, cols * width) if flat else (cols, rows, width)
    dma = pltpu.SemaphoreType.DMA
    far, own, full = pl.pallas_call(
        functools.partial(gather_kernel, cols, group, halves),
        out_shape=(
            jax.ShapeDtypeStruct((group,) + shape, jnp.float32),
            jax.ShapeDtypeStruct(shape, jnp.float32),
            jax.ShapeDtypeStruct((deep, row_total * tall, tile), jnp.float32),
        ),
        in_specs=[VMEM_SPEC, VMEM_SPEC],
        out_specs=(VMEM_SPEC, VMEM_SPEC, VMEM_SPEC),
        scratch_shapes=[
            pltpu.VMEM((cols, rows, width), jnp.float32),
            dma((2, cols, halves)),
            dma((cols, halves)),
            dma((cols, halves)),
            dma((cols, halves)),
            dma((group, cols, halves)),
            dma((group, cols, halves)),
            dma((cols,)),
            dma((cols,)),
            dma((cols,)),
            dma((2, cols)),
            dma((cols,)),
            dma((group, cols)),
            dma((group, cols)),
            dma((group, cols)),
            dma((group, cols)),
        ],
        compiler_params=pltpu.CompilerParams(
            collective_id=0, has_side_effects=True, vmem_limit_bytes=VMEM_BYTES
        ),
    )(panels, window)
    if not flat:
        far = jnp.swapaxes(far, 1, 2)
        own = jnp.swapaxes(own, 0, 1)
    return far.reshape(group * rows, cols * width), own.reshape(rows, cols * width), full


def exchange_kernel(axis, total, add, x_ref, out_ref, held, send_sem, recv_sem):
    me = lax.axis_index(axis)
    barrier = pltpu.get_barrier_semaphore()
    for k in range(1, total):
        pl.semaphore_signal(
            barrier, inc=1, device_id={axis: (me + k) % total}, device_id_type=MESH
        )
    pl.semaphore_wait(barrier, total - 1)
    copies = []
    for k in range(1, total):
        to = (me + k) % total
        copy = pltpu.make_async_remote_copy(
            src_ref=x_ref.at[to], dst_ref=held.at[k - 1], send_sem=send_sem.at[k - 1],
            recv_sem=recv_sem.at[k - 1], device_id={axis: to}, device_id_type=MESH,
        )
        copy.start()
        copies.append(copy)
    if add:
        out_ref[...] = x_ref[me]
    else:
        out_ref[me] = x_ref[me]
    for k in range(1, total):
        copies[k - 1].wait_recv()
        if add:
            out_ref[...] += held[k - 1]
        else:
            out_ref[(me + total - k) % total] = held[k - 1]
    for copy in copies:
        copy.wait_send()


def exchange(x, axis, add, collective_id):
    total = x.shape[0]
    out = x.shape[1:] if add else x.shape
    return pl.pallas_call(
        functools.partial(exchange_kernel, axis, total, add),
        out_shape=jax.ShapeDtypeStruct(out, jnp.float32),
        in_specs=[VMEM_SPEC],
        out_specs=VMEM_SPEC,
        scratch_shapes=[
            pltpu.VMEM((total - 1,) + x.shape[1:], jnp.float32),
            pltpu.SemaphoreType.DMA((total - 1,)),
            pltpu.SemaphoreType.DMA((total - 1,)),
        ],
        compiler_params=pltpu.CompilerParams(
            collective_id=collective_id, has_side_effects=True, vmem_limit_bytes=VMEM_BYTES
        ),
    )(x)


def split(array):
    high = array.astype(jnp.bfloat16)
    return high, (array - high.astype(jnp.float32)).astype(jnp.bfloat16)


def dot_split(left, right):
    out = jnp.dot(left[0], right[1], preferred_element_type=jnp.float32)
    out += jnp.dot(left[1], right[0], preferred_element_type=jnp.float32)
    return out + jnp.dot(left[0], right[0], preferred_element_type=jnp.float32)


def exact(left, right):
    return jnp.dot(left, right, precision=HIGHEST, preferred_element_type=jnp.float32)


def diagonal_inverses(tiles):
    base = tiles[0].shape[0]
    at_row = lax.broadcasted_iota(jnp.int32, (base, base), 0)
    at_col = lax.broadcasted_iota(jnp.int32, (base, base), 1)

    def below(level):
        apart = (at_row >> (level + 1)) == (at_col >> (level + 1))
        return jnp.logical_and(apart, (at_row >> level) > (at_col >> level))

    inverses = []
    for tile in tiles:
        diag = jnp.where(at_row == at_col, tile, 0.0)
        down = 1.0 / jnp.sum(diag, axis=1, keepdims=True)
        over = 1.0 / jnp.sum(diag, axis=0, keepdims=True)
        first = jnp.where(below(0), tile, 0.0) * down * over
        inverses.append(jnp.where(at_row == at_col, down, 0.0) - first)
    level = 1
    while (1 << level) < base:
        mask = below(level)
        lows = [exact(inv, jnp.where(mask, tile, 0.0)) for inv, tile in zip(inverses, tiles)]
        inverses = [inv - exact(low, inv) for inv, low in zip(inverses, lows)]
        level += 1
    return inverses


def images_kernel(
    cols, z_ref, far_ref, win_ref, solved_ref, inva_ref, second_ref,
    far_high, far_low, parts, mated, landed, sums, msend, mrecv, ysend, yrecv,
):
    c = lax.axis_index("col")
    parity = c % 2
    mate = c + 1 - 2 * parity
    pairs = cols // 2
    pair = c // 2
    share = z_ref.shape[0] // cols
    tile = win_ref.shape[1]
    barrier = pltpu.get_barrier_semaphore()
    pl.semaphore_signal(barrier, inc=1, device_id={"col": mate}, device_id_type=MESH)
    for k in range(1, pairs):
        to = (c + 2 * k) % cols
        pl.semaphore_signal(barrier, inc=1, device_id={"col": to}, device_id_type=MESH)

    far_high[...], far_low[...] = split(far_ref[...])

    def partial(column):
        rows = z_ref[pl.ds(pl.multiple_of(column * share, share), share), :]
        return dot_split(split(rows), (far_high[...], far_low[...]))

    def to_mate(k, target):
        copy = pltpu.make_async_remote_copy(
            src_ref=parts.at[k], dst_ref=mated.at[k], send_sem=msend.at[k], recv_sem=mrecv.at[k],
            device_id={"col": target}, device_id_type=MESH,
        )
        copy.start()
        return copy

    mates = []
    crossed = []
    order = [*range(1, pairs), 0]
    for place, k in enumerate(order):
        other = (pair + k) % pairs
        parts[k] = partial(2 * other + 1 - parity)
        if place == 0:
            pl.semaphore_wait(barrier, pairs)
        mates.append(to_mate(k, mate))
    for place, k in enumerate(order):
        other = (pair + k) % pairs
        mine = partial(2 * other + parity)
        mates[place].wait_recv()
        sums[k] = mine + mated[k]
        if k:
            copy = pltpu.make_async_remote_copy(
                src_ref=sums.at[k], dst_ref=landed.at[k], send_sem=ysend.at[k],
                recv_sem=yrecv.at[k], device_id={"col": 2 * other + parity}, device_id_type=MESH,
            )
            copy.start()
            crossed.append(copy)

    base = min(256, tile)
    count = tile // base
    tiles = [
        win_ref[which, i * base : (i + 1) * base, i * base : (i + 1) * base]
        for which in range(2)
        for i in range(count)
    ]
    blocks = diagonal_inverses(tiles)
    second_ref[...] = jnp.zeros_like(second_ref)
    inva_ref[...] = jnp.zeros_like(inva_ref)

    def place_inverse(which, out_ref, offset):
        mine = blocks[which * count : (which + 1) * count]
        for i in range(count):
            out_ref[offset + i * base : offset + (i + 1) * base, i * base : (i + 1) * base] = mine[i]
        for i in range(1, count):
            wide = i * base
            low = win_ref[which, wide : wide + base, :wide]
            above = out_ref[offset : offset + wide, :wide]
            out_ref[offset + wide : offset + wide + base, :wide] = -exact(exact(mine[i], low), above)

    place_inverse(0, inva_ref, 0)
    place_inverse(1, second_ref, tile)
    second_ref[:tile, :] = -exact(exact(inva_ref[...], win_ref[2]), second_ref[tile:, :])
    inv_a = split(inva_ref[...])
    second = split(second_ref[...])

    total = sums[0]
    for place in range(pairs - 1):
        crossed[place].wait_recv()
        total += landed[order[place]]
    high, low = split(total)
    solved_ref[:, :tile] = dot_split((high[:, :tile], low[:, :tile]), inv_a)
    solved_ref[:, tile:] = dot_split((high, low), second)
    for copy in mates + crossed:
        copy.wait_send()


def images_and_inverses(ztrail, far_rows, window, cols):
    share = ztrail.shape[0] // cols
    depth, wide = far_rows.shape
    tile = window.shape[1]
    pairs = cols // 2
    dma = pltpu.SemaphoreType.DMA
    return pl.pallas_call(
        functools.partial(images_kernel, cols),
        out_shape=(
            jax.ShapeDtypeStruct((share, wide), jnp.float32),
            jax.ShapeDtypeStruct((tile, tile), jnp.float32),
            jax.ShapeDtypeStruct((2 * tile, tile), jnp.float32),
        ),
        in_specs=[VMEM_SPEC] * 3,
        out_specs=(VMEM_SPEC,) * 3,
        scratch_shapes=[
            pltpu.VMEM((depth, wide), jnp.bfloat16),
            pltpu.VMEM((depth, wide), jnp.bfloat16),
            *[pltpu.VMEM((pairs, share, wide), jnp.float32)] * 4,
            *[dma((pairs,))] * 4,
        ],
        compiler_params=pltpu.CompilerParams(
            collective_id=1, has_side_effects=True, vmem_limit_bytes=VMEM_BYTES
        ),
    )(ztrail, far_rows, window)


def local(ztrail, panels, window_tiles):
    row_total = lax.axis_size("row")
    cols = lax.axis_size("col")
    col_index = lax.axis_index("col")
    tile = window_tiles.shape[2]
    far_rows, own_rows, window = gather_all(panels, window_tiles, row_total, cols)
    share = ztrail.shape[0] // cols
    solved, inv_a, second = images_and_inverses(ztrail, far_rows, window, cols)
    inv_ab = second[:tile]
    inv_b = second[tile:]
    solved_a = solved[:, :tile]
    solved_b = solved[:, tile:]

    block = tile // cols
    pieces = jnp.stack([solved_a.reshape(share, cols, block), solved_b.reshape(share, cols, block)], 2)
    pieces = jnp.swapaxes(pieces.reshape(share, cols, 2 * block), 0, 1)
    row_solved = exchange(pieces, "col", False, 2).reshape(cols * share, 2 * block)

    def cut(array):
        return lax.dynamic_slice_in_dim(array, col_index * block, block, 1)

    part = 1.0 / row_total
    cut_ab = cut(inv_ab) * part
    inner_a = dot(own_rows[:, :tile], row_solved, ((0,), (0,)))
    inner_a = inner_a + jnp.concatenate([cut(inv_a) * part, cut_ab], 1)
    inner_b = dot(own_rows[:, tile:], row_solved[:, block:], ((0,), (0,))) + cut(inv_b) * part
    tiles_a = dot(inv_a, inner_a, ((0,), (0,)))
    tile_bb = dot(second, jnp.concatenate([inner_a[:, block:], inner_b], 0), ((0,), (0,)))
    corner = jnp.stack([tiles_a[:, :block], tiles_a[:, block:], tile_bb], 0)
    corner = corner.reshape(3, row_total, tile // row_total, block)
    corner_block = exchange(jnp.swapaxes(corner, 0, 1), "row", True, 3)
    return (-solved_a, -solved_b, corner_block)


def solution(mesh):
    placed = (P("row", "col"), P("row", "col"), P(None, "row", None))
    return jax.shard_map(
        local,
        mesh=mesh,
        in_specs=placed,
        out_specs=(P(("row", "col"), None), P(("row", "col"), None), P(None, "row", "col")),
        check_vma=False,
    )
```

```python
import functools

import jax
import jax.numpy as jnp
from jax import lax
from jax.experimental import pallas as pl
from jax.experimental.pallas import tpu as pltpu
from jax.sharding import PartitionSpec as P

HIGHEST = lax.Precision.HIGHEST
HIGH = lax.Precision.HIGH
MESH = pl.DeviceIdType.MESH
VMEM_SPEC = pl.BlockSpec(memory_space=pltpu.VMEM)
VMEM_BYTES = 48 * 1024 * 1024


def dot(left, right, dims=((1,), (0,)), precision=HIGH):
    return lax.dot_general(
        left, right, (dims, ((), ())), precision=precision, preferred_element_type=jnp.float32
    )


def gather_kernel(
    cols, group, halves, p_ref, w_ref, far_ref, own_ref, win_ref, zbuf,
    zsend, zrecv, ysend, yrecv, xsend, xrecv, osend, orecv, ofwd,
    wzsend, wzrecv, wxsend, wxrecv, wdsend, wdrecv,
):
    rows, width = p_ref.shape
    part = rows // halves
    r = lax.axis_index("row")
    c = lax.axis_index("col")
    g = r // group
    j = r % group
    flat = width % 128 == 0

    def slot(ref, column):
        if flat:
            return ref.at[:, pl.ds(pl.multiple_of(column * width, width), width)]
        return ref.at[column]

    def far_at(jj, column, h):
        return slot(far_ref.at[jj], column).at[pl.ds(h * part, part)]

    barrier = pltpu.get_barrier_semaphore()

    def greet(row, col):
        pl.semaphore_signal(barrier, inc=1, device_id=(row, col), device_id_type=MESH)

    for k in range(1, cols):
        greet(r, (c + k) % cols)
    for k in range(1, group):
        greet(g * group + (j + k) % group, c)
    has_left = g > 0
    has_right = g < cols - 1
    pl.when(has_left)(lambda: greet(r - group, c))
    pl.when(has_right)(lambda: greet(r + group, c))
    edges = has_left.astype(jnp.int32) + has_right.astype(jnp.int32)
    pl.semaphore_wait(barrier, cols - 1 + group - 1 + edges)

    pending = []

    def send(cond, src, dst, ssem, rsem, row, col):
        copy = pltpu.make_async_remote_copy(
            src_ref=src, dst_ref=dst, send_sem=ssem, recv_sem=rsem,
            device_id=(row, col), device_id_type=MESH,
        )
        if cond is None:
            copy.start()
        else:
            pl.when(cond)(copy.start)
        pending.append((cond, copy))

    def await_recv(dst, rsem):
        pltpu.make_async_copy(dst, dst, rsem).wait()

    def spread_x(cond, src, column, h):
        for k in range(1, group):
            jj = (j + k) % group
            send(cond, src, far_at(j, column, h), xsend.at[k, column, h],
                 xrecv.at[j, column, h], g * group + jj, c)

    def deliver(cond, src, gs, h):
        remote = gs != c
        local = gs == c
        if cond is not None:
            remote = jnp.logical_and(cond, remote)
            local = jnp.logical_and(cond, local)
        send(remote, src, far_at(j, c, h), ysend.at[gs, h], yrecv.at[c, h], r, gs)
        spread_x(local, src, c, h)

        def keep():
            far_at(j, c, h)[...] = src[...]

        pl.when(local)(keep)

    def relay_x(step):
        mine = jnp.logical_or(g - step == c, g + step == c)
        for h in range(halves):
            for k in range(1, cols):
                column = (c + k) % cols
                block = far_at(j, column, h)
                pl.when(mine)(functools.partial(await_recv, block, yrecv.at[column, h]))
                spread_x(mine, block, column, h)

    for h in range(halves):
        block = p_ref.at[pl.ds(h * part, part)]
        send(has_right, block, zbuf.at[g, pl.ds(h * part, part)], zsend.at[0, g, h],
             zrecv.at[g, h], r + group, c)
        send(has_left, block, zbuf.at[g, pl.ds(h * part, part)], zsend.at[1, g, h],
             zrecv.at[g, h], r - group, c)
    for h in range(halves):
        deliver(None, p_ref.at[pl.ds(h * part, part)], g, h)

    parity = c % 2
    mate = c + 1 - 2 * parity
    tall = w_ref.shape[1]
    half_lanes = w_ref.shape[2] // 2

    def lanes(side):
        return pl.ds(pl.multiple_of(side * half_lanes, half_lanes), half_lanes)

    def win_at(gg, jj, side):
        start = pl.multiple_of((gg * group + jj) * tall, tall)
        return win_ref.at[:, pl.ds(start, tall), lanes(side)]

    def spread_win(cond, src, gg):
        for k in range(1, group):
            send(cond, src, win_at(gg, j, parity), wxsend.at[k, gg], wxrecv.at[j, gg],
                 g * group + (j + k) % group, c)

    own_win = w_ref.at[:, :, lanes(parity)]
    spread_win(None, own_win, g)
    win_ref[:, pl.ds(pl.multiple_of(r * tall, tall), tall), :] = w_ref[...]
    for step in range(1, cols):
        for h in range(halves):
            for side in range(2):
                gs = g - step if side == 0 else g + step
                there = gs >= 0 if side == 0 else gs < cols
                onward = jnp.logical_and(there, has_right if side == 0 else has_left)
                gs = jnp.clip(gs, 0, cols - 1)
                block = zbuf.at[gs, pl.ds(h * part, part)]
                pl.when(there)(functools.partial(await_recv, block, zrecv.at[gs, h]))
                send(onward, block, block, zsend.at[side, gs, h], zrecv.at[gs, h],
                     r + group if side == 0 else r - group, c)
                deliver(there, block, gs, h)
        if step == 1:
            for k in range(0, cols, 2):
                to = (c + k) % cols if k else mate
                send(None, p_ref, slot(own_ref, c), osend.at[k], orecv.at[c], r, to)
            slot(own_ref, c)[...] = p_ref[...]
        if step < cols - 1:
            relay_x(step - 1)
    for k in range(group):
        jj = (j + k) % group
        block = win_at(g, jj, parity)
        if k:
            await_recv(block, wxrecv.at[jj, g])
            send(None, block, block, wdsend.at[jj, g], wdrecv.at[jj, g], r, mate)
        first = block if k else own_win
        send(has_right, first, block, wzsend.at[0, jj, g], wzrecv.at[jj, g], r + group, c)
        send(has_left, first, block, wzsend.at[1, jj, g], wzrecv.at[jj, g], r - group, c)
    relay_x(cols - 2)
    relay_x(cols - 1)
    for step in range(1, cols):
        for k in range(group):
            jj = (j + k) % group
            for side in range(2):
                gs = g - step if side == 0 else g + step
                there = gs >= 0 if side == 0 else gs < cols
                onward = jnp.logical_and(there, has_right if side == 0 else has_left)
                gs = jnp.clip(gs, 0, cols - 1)
                block = win_at(gs, jj, parity)
                pl.when(there)(functools.partial(await_recv, block, wzrecv.at[jj, gs]))
                send(onward, block, block, wzsend.at[side, jj, gs], wzrecv.at[jj, gs],
                     r + group if side == 0 else r - group, c)
                send(there, block, block, wdsend.at[jj, gs], wdrecv.at[jj, gs], r, mate)
    for k in range(2, cols, 2):
        column = (c + k) % cols
        block = slot(own_ref, column)
        await_recv(block, orecv.at[column])
        send(None, block, block, ofwd.at[column], orecv.at[column], r, mate)
    for k in range(0, cols, 2):
        column = (mate + k) % cols
        await_recv(slot(own_ref, column), orecv.at[column])
    for k in range(1, cols):
        gg = (g + k) % cols
        await_recv(win_at(gg, j, 1 - parity), wdrecv.at[j, gg])
    for k in range(1, group):
        jj = (j + k) % group
        for gg in range(cols):
            await_recv(win_at(gg, jj, 1 - parity), wdrecv.at[jj, gg])
    for k in range(1, group):
        jj = (j + k) % group
        for column in range(cols):
            for h in range(halves):
                await_recv(far_at(jj, column, h), xrecv.at[jj, column, h])
    for cond, copy in pending:
        if cond is None:
            copy.wait_send()
        else:
            pl.when(cond)(copy.wait_send)


def gather_all(panels, window, row_total, cols):
    rows, width = panels.shape
    deep, tall, tile = window.shape
    group = row_total // cols
    halves = 2
    flat = width % 128 == 0
    shape = (rows, cols * width) if flat else (cols, rows, width)
    dma = pltpu.SemaphoreType.DMA
    far, own, full = pl.pallas_call(
        functools.partial(gather_kernel, cols, group, halves),
        out_shape=(
            jax.ShapeDtypeStruct((group,) + shape, jnp.float32),
            jax.ShapeDtypeStruct(shape, jnp.float32),
            jax.ShapeDtypeStruct((deep, row_total * tall, tile), jnp.float32),
        ),
        in_specs=[VMEM_SPEC, VMEM_SPEC],
        out_specs=(VMEM_SPEC, VMEM_SPEC, VMEM_SPEC),
        scratch_shapes=[
            pltpu.VMEM((cols, rows, width), jnp.float32),
            dma((2, cols, halves)),
            dma((cols, halves)),
            dma((cols, halves)),
            dma((cols, halves)),
            dma((group, cols, halves)),
            dma((group, cols, halves)),
            dma((cols,)),
            dma((cols,)),
            dma((cols,)),
            dma((2, group, cols)),
            dma((group, cols)),
            dma((group, cols)),
            dma((group, cols)),
            dma((group, cols)),
            dma((group, cols)),
        ],
        compiler_params=pltpu.CompilerParams(
            collective_id=0, has_side_effects=True, vmem_limit_bytes=VMEM_BYTES
        ),
    )(panels, window)
    if not flat:
        far = jnp.swapaxes(far, 1, 2)
        own = jnp.swapaxes(own, 0, 1)
    return far.reshape(group * rows, cols * width), own.reshape(rows, cols * width), full


def exchange_kernel(axis, total, add, x_ref, out_ref, held, send_sem, recv_sem):
    me = lax.axis_index(axis)
    barrier = pltpu.get_barrier_semaphore()
    for k in range(1, total):
        pl.semaphore_signal(
            barrier, inc=1, device_id={axis: (me + k) % total}, device_id_type=MESH
        )
    pl.semaphore_wait(barrier, total - 1)
    copies = []
    for k in range(1, total):
        to = (me + k) % total
        copy = pltpu.make_async_remote_copy(
            src_ref=x_ref.at[to], dst_ref=held.at[k - 1], send_sem=send_sem.at[k - 1],
            recv_sem=recv_sem.at[k - 1], device_id={axis: to}, device_id_type=MESH,
        )
        copy.start()
        copies.append(copy)
    if add:
        out_ref[...] = x_ref[me]
    else:
        out_ref[me] = x_ref[me]
    for k in range(1, total):
        copies[k - 1].wait_recv()
        if add:
            out_ref[...] += held[k - 1]
        else:
            out_ref[(me + total - k) % total] = held[k - 1]
    for copy in copies:
        copy.wait_send()


def exchange(x, axis, add, collective_id):
    total = x.shape[0]
    out = x.shape[1:] if add else x.shape
    return pl.pallas_call(
        functools.partial(exchange_kernel, axis, total, add),
        out_shape=jax.ShapeDtypeStruct(out, jnp.float32),
        in_specs=[VMEM_SPEC],
        out_specs=VMEM_SPEC,
        scratch_shapes=[
            pltpu.VMEM((total - 1,) + x.shape[1:], jnp.float32),
            pltpu.SemaphoreType.DMA((total - 1,)),
            pltpu.SemaphoreType.DMA((total - 1,)),
        ],
        compiler_params=pltpu.CompilerParams(
            collective_id=collective_id, has_side_effects=True, vmem_limit_bytes=VMEM_BYTES
        ),
    )(x)


def split(array):
    high = array.astype(jnp.bfloat16)
    return high, (array - high.astype(jnp.float32)).astype(jnp.bfloat16)


def dot_split(left, right):
    out = jnp.dot(left[0], right[1], preferred_element_type=jnp.float32)
    out += jnp.dot(left[1], right[0], preferred_element_type=jnp.float32)
    return out + jnp.dot(left[0], right[0], preferred_element_type=jnp.float32)


def exact(left, right):
    return jnp.dot(left, right, precision=HIGHEST, preferred_element_type=jnp.float32)


def diagonal_inverses(tiles):
    base = tiles[0].shape[0]
    at_row = lax.broadcasted_iota(jnp.int32, (base, base), 0)
    at_col = lax.broadcasted_iota(jnp.int32, (base, base), 1)

    def below(level):
        apart = (at_row >> (level + 1)) == (at_col >> (level + 1))
        return jnp.logical_and(apart, (at_row >> level) > (at_col >> level))

    inverses = []
    for tile in tiles:
        diag = jnp.where(at_row == at_col, tile, 0.0)
        down = 1.0 / jnp.sum(diag, axis=1, keepdims=True)
        over = 1.0 / jnp.sum(diag, axis=0, keepdims=True)
        first = jnp.where(below(0), tile, 0.0) * down * over
        inverses.append(jnp.where(at_row == at_col, down, 0.0) - first)
    level = 1
    while (1 << level) < base:
        mask = below(level)
        lows = [exact(inv, jnp.where(mask, tile, 0.0)) for inv, tile in zip(inverses, tiles)]
        inverses = [inv - exact(low, inv) for inv, low in zip(inverses, lows)]
        level += 1
    return inverses


def images_kernel(
    cols, z_ref, far_ref, win_ref, solved_ref, inva_ref, second_ref,
    far_high, far_low, parts, mated, landed, sums, msend, mrecv, ysend, yrecv,
):
    c = lax.axis_index("col")
    parity = c % 2
    mate = c + 1 - 2 * parity
    pairs = cols // 2
    pair = c // 2
    share = z_ref.shape[0] // cols
    tile = win_ref.shape[1]
    barrier = pltpu.get_barrier_semaphore()
    pl.semaphore_signal(barrier, inc=1, device_id={"col": mate}, device_id_type=MESH)
    for k in range(1, pairs):
        to = (c + 2 * k) % cols
        pl.semaphore_signal(barrier, inc=1, device_id={"col": to}, device_id_type=MESH)

    far_high[...], far_low[...] = split(far_ref[...])

    def partial(column):
        rows = z_ref[pl.ds(pl.multiple_of(column * share, share), share), :]
        return dot_split(split(rows), (far_high[...], far_low[...]))

    def to_mate(k, target):
        copy = pltpu.make_async_remote_copy(
            src_ref=parts.at[k], dst_ref=mated.at[k], send_sem=msend.at[k], recv_sem=mrecv.at[k],
            device_id={"col": target}, device_id_type=MESH,
        )
        copy.start()
        return copy

    mates = []
    crossed = []
    order = [*range(1, pairs), 0]
    for place, k in enumerate(order):
        other = (pair + k) % pairs
        parts[k] = partial(2 * other + 1 - parity)
        if place == 0:
            pl.semaphore_wait(barrier, pairs)
        mates.append(to_mate(k, mate))
    for place, k in enumerate(order):
        other = (pair + k) % pairs
        mine = partial(2 * other + parity)
        mates[place].wait_recv()
        sums[k] = mine + mated[k]
        if k:
            copy = pltpu.make_async_remote_copy(
                src_ref=sums.at[k], dst_ref=landed.at[k], send_sem=ysend.at[k],
                recv_sem=yrecv.at[k], device_id={"col": 2 * other + parity}, device_id_type=MESH,
            )
            copy.start()
            crossed.append(copy)

    base = min(256, tile)
    count = tile // base
    tiles = [
        win_ref[which, i * base : (i + 1) * base, i * base : (i + 1) * base]
        for which in range(2)
        for i in range(count)
    ]
    blocks = diagonal_inverses(tiles)
    second_ref[...] = jnp.zeros_like(second_ref)
    inva_ref[...] = jnp.zeros_like(inva_ref)

    def place_inverse(which, out_ref, offset):
        mine = blocks[which * count : (which + 1) * count]
        for i in range(count):
            out_ref[offset + i * base : offset + (i + 1) * base, i * base : (i + 1) * base] = mine[i]
        for i in range(1, count):
            wide = i * base
            low = win_ref[which, wide : wide + base, :wide]
            above = out_ref[offset : offset + wide, :wide]
            out_ref[offset + wide : offset + wide + base, :wide] = -exact(exact(mine[i], low), above)

    place_inverse(0, inva_ref, 0)
    place_inverse(1, second_ref, tile)
    second_ref[:tile, :] = -exact(exact(inva_ref[...], win_ref[2]), second_ref[tile:, :])
    inv_a = split(inva_ref[...])
    second = split(second_ref[...])

    total = sums[0]
    for place in range(pairs - 1):
        crossed[place].wait_recv()
        total += landed[order[place]]
    high, low = split(total)
    solved_ref[:, :tile] = dot_split((high[:, :tile], low[:, :tile]), inv_a)
    solved_ref[:, tile:] = dot_split((high, low), second)
    for copy in mates + crossed:
        copy.wait_send()


def images_and_inverses(ztrail, far_rows, window, cols):
    share = ztrail.shape[0] // cols
    depth, wide = far_rows.shape
    tile = window.shape[1]
    pairs = cols // 2
    dma = pltpu.SemaphoreType.DMA
    return pl.pallas_call(
        functools.partial(images_kernel, cols),
        out_shape=(
            jax.ShapeDtypeStruct((share, wide), jnp.float32),
            jax.ShapeDtypeStruct((tile, tile), jnp.float32),
            jax.ShapeDtypeStruct((2 * tile, tile), jnp.float32),
        ),
        in_specs=[VMEM_SPEC] * 3,
        out_specs=(VMEM_SPEC,) * 3,
        scratch_shapes=[
            pltpu.VMEM((depth, wide), jnp.bfloat16),
            pltpu.VMEM((depth, wide), jnp.bfloat16),
            *[pltpu.VMEM((pairs, share, wide), jnp.float32)] * 4,
            *[dma((pairs,))] * 4,
        ],
        compiler_params=pltpu.CompilerParams(
            collective_id=1, has_side_effects=True, vmem_limit_bytes=VMEM_BYTES
        ),
    )(ztrail, far_rows, window)


def local(ztrail, panels, window_tiles):
    row_total = lax.axis_size("row")
    cols = lax.axis_size("col")
    col_index = lax.axis_index("col")
    tile = window_tiles.shape[2]
    far_rows, own_rows, window = gather_all(panels, window_tiles, row_total, cols)
    share = ztrail.shape[0] // cols
    solved, inv_a, second = images_and_inverses(ztrail, far_rows, window, cols)
    inv_ab = second[:tile]
    inv_b = second[tile:]
    solved_a = solved[:, :tile]
    solved_b = solved[:, tile:]

    block = tile // cols
    pieces = jnp.stack([solved_a.reshape(share, cols, block), solved_b.reshape(share, cols, block)], 2)
    pieces = jnp.swapaxes(pieces.reshape(share, cols, 2 * block), 0, 1)
    row_solved = exchange(pieces, "col", False, 2).reshape(cols * share, 2 * block)

    def cut(array):
        return lax.dynamic_slice_in_dim(array, col_index * block, block, 1)

    part = 1.0 / row_total
    cut_ab = cut(inv_ab) * part
    inner_a = dot(own_rows[:, :tile], row_solved, ((0,), (0,)))
    inner_a = inner_a + jnp.concatenate([cut(inv_a) * part, cut_ab], 1)
    inner_b = dot(own_rows[:, tile:], row_solved[:, block:], ((0,), (0,))) + cut(inv_b) * part
    tiles_a = dot(inv_a, inner_a, ((0,), (0,)))
    tile_bb = dot(second, jnp.concatenate([inner_a[:, block:], inner_b], 0), ((0,), (0,)))
    corner = jnp.stack([tiles_a[:, :block], tiles_a[:, block:], tile_bb], 0)
    corner = corner.reshape(3, row_total, tile // row_total, block)
    corner_block = exchange(jnp.swapaxes(corner, 0, 1), "row", True, 3)
    return (-solved_a, -solved_b, corner_block)


def solution(mesh):
    placed = (P("row", "col"), P("row", "col"), P(None, "row", None))
    return jax.shard_map(
        local,
        mesh=mesh,
        in_specs=placed,
        out_specs=(P(("row", "col"), None), P(("row", "col"), None), P(None, "row", "col")),
        check_vma=False,
    )
```
